32 devices in a mesh: snap: 2 (over x), node: 16 (over z, y, core).
Axes of the slice: x: 2, y: 2, z: 4, core: 2. Of those that a mesh axis runs over, the one named last changes fastest.
Arguments:
- features: bfloat16 [2, 16384, 512], P('snap', 'node'), may hold values from -6 to 6
- tile_rows: int32 [2, 448], P('snap', 'node'), may hold values from 0 to 127, as said below
- tile_cols: int32 [2, 448], P('snap', 'node'), may hold values from 0 to 127, as said below
- tile_values: bfloat16 [2, 448, 128, 128], P('snap', 'node'), may hold values from -0.125 to 0.125
- tile_count: int32 [2, 16], P('snap', 'node'), may hold values from 9 to 28, as said below
- w_graph: bfloat16 [512, 512], replicated, may hold values from -0.25 to 0.25
- norm_gain: float32 [512], replicated, may hold values from 0.5 to 1.5
- w_query: bfloat16 [512, 512], replicated
- w_key: bfloat16 [512, 512], replicated, may hold values from -0.25 to 0.25
- w_value: bfloat16 [512, 512], replicated, may hold values from -0.25 to 0.25
- w_out: bfloat16 [512, 512], replicated, may hold values from -0.25 to 0.25
Outputs:
- layer_out: bfloat16 [2, 16384, 512], P(None, ('node', 'snap'))
The draws below stay inside these ranges and needn't reach their ends.
Inputs may be any that keep to these rules, and one draw needn't show every extreme that they name: `tile_rows`: every slot held by node index j (slots j * 28 to (j + 1) * 28 - 1) names a row block of that index's own nodes. `tile_cols`: every slot held by node index j names a column block of the nodes held by node indices j - 2 to j + 2. Of each node index's slots, the first tile_count are live and the rest are ignored; in each snapshot some node index has all 28 live.
All inputs are finite; a program needn't handle non-finite values.
Results may differ from the reference program's by a relative error of at most 0.0086.
Values may be sent and summed in bfloat16 or wider, within the bound.
No kernel may reach another device: no remote copies, remote signals or barrier semaphores. Data moves between devices by JAX's collectives and lax.ppermute only.
A program may use at most 64 MiB of HBM per device.

```python
import jax
import jax.numpy as jnp
from jax import lax

D = 512
HEADS = 8
HEAD_DIM = 64
TILE = 128
NODE_DEV = 1024
TILE_DEV = 28
SNAPS = 2
NODES = 16384
TILES = 448


def draw_tile_rows(key, part):
    slots = jnp.arange(TILES)
    device = slots // TILE_DEV
    blocks_dev = NODE_DEV // TILE
    local = jax.random.randint(jax.random.fold_in(key, 11), (SNAPS, TILES), 0, blocks_dev)
    return (device[None, :] * blocks_dev + local).astype(jnp.int32)


def draw_tile_cols(key, part):
    key_a, key_b = jax.random.split(jax.random.fold_in(key, 23))
    slots = jnp.arange(TILES)
    device = slots // TILE_DEV
    within = slots % TILE_DEV
    blocks_dev = NODE_DEV // TILE
    devices = TILES // TILE_DEV
    offset = jax.random.randint(key_a, (SNAPS, TILES), -2, 3)
    offset = jnp.where(within[None, :] < 5, within[None, :] - 2, offset)
    target = jnp.clip(device[None, :] + offset, 0, devices - 1)
    local = jax.random.randint(key_b, (SNAPS, TILES), 0, blocks_dev)
    return (target * blocks_dev + local).astype(jnp.int32)


def draw_tile_count(key, part):
    key_a, key_b = jax.random.split(jax.random.fold_in(key, 37))
    devices = TILES // TILE_DEV
    low = max(5, TILE_DEV // 3)
    count = jax.random.randint(key_a, (SNAPS, devices), low, TILE_DEV + 1)
    full = jax.random.randint(key_b, (SNAPS, 1), 0, devices)
    count = jnp.where(jnp.arange(devices)[None, :] == full, TILE_DEV, count)
    return count.astype(jnp.int32)


def draw_w_query(key, part):
    key_a = jax.random.fold_in(jax.random.fold_in(key, 53), 0)
    base = jax.random.normal(key_a, (D, D), jnp.float32) * D ** (-0.5)
    return base.astype(jnp.bfloat16)


def shard_levels(key, extent, cuts, least, largest):
    gain = 1.0
    for position, shards_of in cuts:
        draws = jax.random.uniform(jax.random.fold_in(jax.random.fold_in(key, 6), position), (shards_of,), jnp.float32, least / len(cuts), largest / len(cuts))
        gain = gain * jnp.repeat(jnp.exp(draws), extent[position] // shards_of).reshape((-1,) + (1,) * (len(extent) - 1 - position))
    return gain


def normal_values(own_key, shape, scale, limit, shards=(), kind=jnp.bfloat16):
    values = jax.random.normal(own_key, shape, jnp.float32) * scale
    if len(shards) > 0:
        values = shard_levels(own_key, shape, shards, -0.22, 0.18) * values
    return jnp.clip(values, min=-limit, max=limit).astype(kind)


def setup_inputs(seed: int = 0) -> dict:
    streams_of = jax.random.split(jax.random.key(seed), 12)
    return {
        "features": normal_values(streams_of[0], (SNAPS, NODES, D), 1.0, 6.0, ((0, 2), (1, 16))),
        "tile_rows": draw_tile_rows(jax.random.fold_in(streams_of[11], 71), 0),
        "tile_cols": draw_tile_cols(jax.random.fold_in(streams_of[11], 71), 0),
        "tile_values": normal_values(streams_of[3], (SNAPS, TILES, TILE, TILE), (TILE_DEV * 64) ** -0.5, 0.125, ((0, 2), (1, 16))),
        "tile_count": draw_tile_count(jax.random.fold_in(streams_of[11], 71), 0),
        "w_graph": normal_values(streams_of[5], (D, D), D ** -0.5, 0.25),
        "norm_gain": jnp.clip(1.0 + 0.1 * jax.random.normal(streams_of[6], (D,), jnp.float32), 0.5, 1.5),
        "w_query": draw_w_query(jax.random.fold_in(streams_of[11], 71), 0),
        "w_key": normal_values(streams_of[8], (D, D), D ** -0.5, 0.25),
        "w_value": normal_values(streams_of[9], (D, D), D ** -0.5, 0.25),
        "w_out": normal_values(streams_of[10], (D, D), D ** -0.5, 0.25),
    }


def norm_rows(hidden, norm_gain):
    value = hidden.astype(jnp.float32)
    mean = lax.optimization_barrier(jnp.mean(value, axis=-1, keepdims=True))
    centred = value - mean
    variance = lax.optimization_barrier(jnp.mean(centred * centred, axis=-1, keepdims=True))
    return (centred * lax.rsqrt(variance + 1e-05) * norm_gain).astype(jnp.bfloat16)

def snapshot_graph(feats, rows, cols, values, count, w_graph):
    blocks_dev = NODE_DEV // TILE
    blocks = feats.reshape(NODES // TILE, TILE, D)
    slots = jnp.arange(TILE_DEV).astype(jnp.int32)

    def one_device(carry, item):
        row_ids, col_ids, tiles, live_count, device = item
        picked = blocks[col_ids].astype(jnp.float32)
        prod = jnp.einsum('tij,tjd->tid', tiles.astype(jnp.float32), picked)
        prod = jnp.where((slots < live_count)[:, None, None], prod, jnp.float32(0.0))
        local = (row_ids - device * blocks_dev).astype(jnp.int32)
        summed = jax.ops.segment_sum(prod, local, num_segments=blocks_dev)
        return (carry, summed)
    devices = jnp.arange(NODES // NODE_DEV).astype(jnp.int32)
    unused, sums = lax.scan(one_device, jnp.float32(0.0), (rows, cols, values, count, devices))
    aggregated = sums.reshape(NODES, D).astype(jnp.bfloat16)
    mixed = jnp.dot(aggregated, w_graph, preferred_element_type=jnp.float32)
    return (feats.astype(jnp.float32) + jax.nn.relu(mixed)).astype(jnp.bfloat16)

def reference(features, tile_rows, tile_cols, tile_values, tile_count, w_graph, norm_gain, w_query, w_key, w_value, w_out):
    devices = NODES // NODE_DEV
    rows = tile_rows.reshape(SNAPS, devices, TILE_DEV)
    cols = tile_cols.reshape(SNAPS, devices, TILE_DEV)
    values = tile_values.reshape(SNAPS, devices, TILE_DEV, TILE, TILE)

    def per_snapshot(item):
        feats, row_ids, col_ids, tiles, count = item
        return snapshot_graph(feats, row_ids, col_ids, tiles, count, w_graph)
    hidden = lax.map(per_snapshot, (features, rows, cols, values, tile_count))
    normed = norm_rows(hidden, norm_gain).reshape(SNAPS * NODES, D)
    query = jnp.dot(normed, w_query, preferred_element_type=jnp.float32).astype(jnp.bfloat16)
    key = jnp.dot(normed, w_key, preferred_element_type=jnp.float32).astype(jnp.bfloat16)
    value = jnp.dot(normed, w_value, preferred_element_type=jnp.float32).astype(jnp.bfloat16)
    query = query.reshape(SNAPS, NODES, HEADS, HEAD_DIM).astype(jnp.float32)
    key = key.reshape(SNAPS, NODES, HEADS, HEAD_DIM).astype(jnp.float32)
    value = value.reshape(SNAPS, NODES, HEADS, HEAD_DIM).astype(jnp.float32)
    scores = jnp.einsum('snhd,unhd->nhsu', query, key) * HEAD_DIM ** (-0.5)
    later = jnp.arange(SNAPS)[:, None] >= jnp.arange(SNAPS)[None, :]
    scores = jnp.where(later, scores, jnp.float32(-1e+30))
    weights = jax.nn.softmax(scores, axis=-1).astype(jnp.bfloat16)
    context = jnp.einsum('nhsu,unhd->snhd', weights.astype(jnp.float32), value)
    context = context.astype(jnp.bfloat16).reshape(SNAPS * NODES, D)
    projected = jnp.dot(context, w_out, preferred_element_type=jnp.float32)
    result = hidden.reshape(SNAPS * NODES, D).astype(jnp.float32) + projected
    return result.astype(jnp.bfloat16).reshape(SNAPS, NODES, D)
```

```python
import functools

import jax
import jax.numpy as jnp
from jax import lax
from jax.experimental import pallas as pl
from jax.experimental.pallas import tpu as pltpu
from jax.sharding import PartitionSpec as P

HEAD_DIM = 64
GROUPS = ((0,), (1,), (2,), (3,))
CHUNK = 128

VMEM_SPEC = pl.BlockSpec(memory_space=pltpu.VMEM)
SMEM_SPEC = pl.BlockSpec(memory_space=pltpu.SMEM)


def routes(nodes):
    far = nodes // 4
    across = [(n, n ^ 2) for n in range(nodes)]
    beside = [(n, n ^ 1) for n in range(nodes)]
    onward = []
    for n in range(nodes):
        group, within = divmod(n, 4)
        step = 1 if within < 2 else -1
        onward.append((n, ((group + step) % far) * 4 + within))
    return across, beside, onward


def graph_kernel(blocks_dev, snaps, sources, rows_ref, cols_ref, count_ref, me_ref, tiles_ref, *refs):
    source_refs, refs = refs[:sources], refs[sources:]
    out_refs, (window, total) = refs[:snaps], refs[snaps:]
    slots, tile, _ = tiles_ref.shape
    here = rows_ref[0, 0] // blocks_dev
    lead = (here // 2) % 2
    core = here % 2
    low = 3 - lead
    high = 2 + lead
    order = [
        low,
        jnp.where(core == 0, 4, 1),
        0,
        jnp.where(core == 0, 1, 4),
        high,
    ]
    span = source_refs[0].shape[0] // tile
    for number, ref in enumerate(source_refs):
        for block in range(span):
            window[number * span + block] = ref[block * tile : (block + 1) * tile, :]
    total[...] = jnp.zeros_like(total)
    first = (here - 2) * blocks_dev
    live = count_ref[0, 0]
    for slot in range(slots):
        col = cols_ref[0, slot] - first
        side = col // blocks_dev
        number = order[4]
        for index in range(4):
            number = jnp.where(side == index, order[index], number)
        block = number * span + col % blocks_dev
        row = jnp.where(slot < live, rows_ref[0, slot] - here * blocks_dev, blocks_dev)
        total[row] += jnp.dot(tiles_ref[slot], window[block], preferred_element_type=jnp.float32)
    each = blocks_dev // snaps
    me = me_ref[0]
    for distance, out_ref in enumerate(out_refs):
        part = lax.rem(me + distance, snaps)
        for block in range(each):
            out_ref[block * tile : (block + 1) * tile, :] = total[part * each + block].astype(out_ref.dtype)


def graph_call(rows, cols, count, me, tiles, sources, snaps, blocks_dev):
    width = sources[0].shape[1]
    slots, tile, _ = tiles.shape
    nodes_dev = sources[0].shape[0]
    part = nodes_dev // snaps
    return pl.pallas_call(
        functools.partial(graph_kernel, blocks_dev, snaps, len(sources)),
        out_shape=[jax.ShapeDtypeStruct((part, width), jnp.bfloat16)] * snaps,
        in_specs=[SMEM_SPEC] * 4 + [VMEM_SPEC] * (1 + len(sources)),
        out_specs=[VMEM_SPEC] * snaps,
        scratch_shapes=[
            pltpu.VMEM((len(sources) * blocks_dev, tile, width), jnp.bfloat16),
            pltpu.VMEM((blocks_dev + 1, tile, width), jnp.float32),
        ],
        compiler_params=pltpu.CompilerParams(vmem_limit_bytes=16 << 20),
        cost_estimate=pl.CostEstimate(
            flops=2 * slots * tile * tile * width, bytes_accessed=4 << 20, transcendentals=0
        ),
        name="graph",
    )(rows, cols, count, me, tiles, *sources)


def layer_kernel(snaps, groups, me_ref, gain_ref, wg_ref, wq_ref, wk_ref, wv_ref, wo_ref, *refs):
    feat_refs, refs = refs[:snaps], refs[snaps:]
    agg_refs, refs = refs[: snaps * groups], refs[snaps * groups :]
    out_ref, hidden, normed, query, key, value, context, heads = refs
    _, part, width = out_ref.shape
    me = me_ref[0]
    gain = gain_ref[...]
    step = min(part, 128)
    for distance in range(snaps):
        snap = lax.rem(me - distance + snaps, snaps)
        feat_ref = feat_refs[distance]
        mine = agg_refs[distance * groups : (distance + 1) * groups]

        @pl.loop(0, part // step)
        def _(index):
            at = pl.ds(pl.multiple_of(index * step, step), step)
            agg = jnp.concatenate([ref[at, :] for ref in mine], axis=1)
            mixed = jnp.dot(agg, wg_ref[...], preferred_element_type=jnp.float32)
            hid = (feat_ref[at, :].astype(jnp.float32) + jnp.maximum(mixed, 0.0)).astype(jnp.bfloat16)
            hidden[snap, at, :] = hid
            val = hid.astype(jnp.float32)
            mean = jnp.mean(val, axis=-1, keepdims=True)
            centred = val - mean
            variance = jnp.mean(centred * centred, axis=-1, keepdims=True)
            normed[snap, at, :] = (centred * lax.rsqrt(variance + 1e-05) * gain).astype(jnp.bfloat16)

    head_row = lax.broadcasted_iota(jnp.int32, (width, width), 0) // HEAD_DIM
    head_col = lax.broadcasted_iota(jnp.int32, (width, width), 1) // HEAD_DIM
    heads[...] = jnp.where(head_row == head_col, 1.0, 0.0).astype(jnp.bfloat16)

    for snap in range(snaps):
        big = min(part, 256)

        @pl.loop(0, part // big)
        def _(index):
            at = pl.ds(pl.multiple_of(index * big, big), big)
            rows = normed[snap, at, :]
            query[snap, at, :] = jnp.dot(rows, wq_ref[...], preferred_element_type=jnp.float32).astype(jnp.bfloat16)
            key[snap, at, :] = jnp.dot(rows, wk_ref[...], preferred_element_type=jnp.float32).astype(jnp.bfloat16)
            value[snap, at, :] = jnp.dot(rows, wv_ref[...], preferred_element_type=jnp.float32).astype(jnp.bfloat16)

    @pl.loop(0, part // step)
    def _(index):
        at = pl.ds(pl.multiple_of(index * step, step), step)
        for snap in range(snaps):
            que = query[snap, at, :].astype(jnp.float32)
            scores = []
            for other in range(snap + 1):
                exact = que * key[other, at, :].astype(jnp.float32)
                high = exact.astype(jnp.bfloat16)
                low = (exact - high.astype(jnp.float32)).astype(jnp.bfloat16)
                score = jnp.dot(high, heads[...], preferred_element_type=jnp.float32)
                score += jnp.dot(low, heads[...], preferred_element_type=jnp.float32)
                scores.append(score * HEAD_DIM**-0.5)
            peak = functools.reduce(jnp.maximum, scores)
            powers = [jnp.exp(score - peak) for score in scores]
            whole = functools.reduce(jnp.add, powers)
            mixed = jnp.zeros_like(whole)
            for other in range(snap + 1):
                weight = (powers[other] / whole).astype(jnp.bfloat16).astype(jnp.float32)
                mixed += weight * value[other, at, :].astype(jnp.float32)
            context[snap, at, :] = mixed.astype(jnp.bfloat16)

    for snap in range(snaps):
        big = min(part, 256)

        @pl.loop(0, part // big)
        def _(index):
            at = pl.ds(pl.multiple_of(index * big, big), big)
            made = jnp.dot(context[snap, at, :], wo_ref[...], preferred_element_type=jnp.float32)
            out_ref[snap, at, :] = (hidden[snap, at, :].astype(jnp.float32) + made).astype(jnp.bfloat16)


def layer_call(me, gain, weights, feats, aggs, snaps):
    part, width = feats[0].shape
    groups = len(aggs) // snaps
    full = (snaps, part, width)
    return pl.pallas_call(
        functools.partial(layer_kernel, snaps, groups),
        out_shape=jax.ShapeDtypeStruct(full, jnp.bfloat16),
        in_specs=[SMEM_SPEC] + [VMEM_SPEC] * (1 + len(weights) + len(feats) + len(aggs)),
        out_specs=VMEM_SPEC,
        scratch_shapes=[pltpu.VMEM(full, jnp.bfloat16)] * 6 + [pltpu.VMEM((width, width), jnp.bfloat16)],
        compiler_params=pltpu.CompilerParams(vmem_limit_bytes=32 << 20),
        cost_estimate=pl.CostEstimate(
            flops=10 * snaps * part * width * width, bytes_accessed=8 << 20, transcendentals=0
        ),
        name="layer",
    )(me, gain, *weights, *feats, *aggs)


def local(
    features,
    tile_rows,
    tile_cols,
    tile_values,
    tile_count,
    w_graph,
    norm_gain,
    w_query,
    w_key,
    w_value,
    w_out,
):
    feats = features[0]
    nodes_dev, width = feats.shape
    tile = tile_values.shape[-1]
    blocks_dev = nodes_dev // tile
    snaps = lax.axis_size("snap")
    part = nodes_dev // snaps
    across, beside, onward = routes(lax.axis_size("node"))
    here = lax.axis_index("node")
    me = lax.axis_index("snap").astype(jnp.int32)
    me_ref = me.reshape(1)
    shifts = [[(i, (i + d) % snaps) for i in range(snaps)] for d in range(snaps)]

    chunks = width // CHUNK
    mine = [feats[:, c * CHUNK : (c + 1) * CHUNK] for c in range(chunks)]
    near = [lax.ppermute(block, "node", across) for block in mine]
    partner = lax.ppermute(feats, "node", beside)
    parts = feats.reshape(snaps, part, width)
    own_feats = [lax.dynamic_index_in_dim(parts, lax.rem(me + d, snaps), 0, keepdims=False) for d in range(snaps)]
    feat_parts = [own_feats[0]] + [lax.ppermute(own_feats[d], "snap", shifts[d]) for d in range(1, snaps)]
    far = [lax.ppermute(block, "node", onward) for block in near]
    same = (here // 2) % 2 == here % 2
    received = [[] for _ in range(snaps)]
    for group in GROUPS:
        join = lambda blocks: jnp.concatenate([blocks[c] for c in group], axis=1)
        close, away = join(near), join(far)
        relayed = lax.ppermute(jnp.where(same, close, away), "node", beside)
        columns = slice(group[0] * CHUNK, (group[-1] + 1) * CHUNK)
        sources = [feats[:, columns], partner[:, columns], close, away, relayed]
        outs = graph_call(tile_rows, tile_cols, tile_count, me_ref, tile_values[0], sources, snaps, blocks_dev)
        received[0].append(outs[0])
        for d in range(1, snaps):
            received[d].append(lax.ppermute(outs[d], "snap", shifts[d]))
    aggs = [agg for rows in received for agg in rows]
    return layer_call(
        me_ref,
        norm_gain.reshape(1, width),
        (w_graph, w_query, w_key, w_value, w_out),
        feat_parts,
        aggs,
        snaps,
    )


def solution(mesh):
    in_specs = (
        P("snap", "node", None),
        P("snap", "node"),
        P("snap", "node"),
        P("snap", "node", None, None),
        P("snap", "node"),
        P(),
        P(),
        P(),
        P(),
        P(),
        P(),
    )
    out_specs = P(None, ("node", "snap"), None)
    return jax.shard_map(local, mesh=mesh, in_specs=in_specs, out_specs=out_specs, check_vma=False)
```
